128 devices in a mesh: bank: 4 (over y_lo, core), zero: 32 (over z, y_hi, x).
Axes of the slice: x: 4, y: 4 (y_hi: 2, y_lo: 2; y = y_hi * 2 + y_lo), z: 4, core: 2. Of those that a mesh axis runs over, the one named last changes fastest.
Arguments:
- train_gate: float32 [128, 2048, 768], P('bank', 'zero'), may hold values from -0.25 to 0.25
- other_gate: bfloat16 [128, 2048, 768], P('bank', 'zero'), may hold values from -0.0625 to 0.0625
- train_up: float32 [128, 2048, 768], P('bank', 'zero'), may hold values from -0.25 to 0.25
- other_up: bfloat16 [128, 2048, 768], P('bank', 'zero'), may hold values from -0.0625 to 0.0625
- router_weight: float32 [2048, 128], P('zero', 'bank'), may hold values from -0.125 to 0.125
- router_gain: float32 [2048], P('zero'), may hold values from 0.25 to 1.75
Outputs:
- ready_gate: bfloat16 [128, 2048, 768], P(('bank', 'zero'))
- ready_up: bfloat16 [128, 2048, 768], P(('bank', 'zero'))
- scale_gate: float32 [128, 768], P(('bank', 'zero'))
- scale_up: float32 [128, 768], P(('bank', 'zero'))
- serve_router: bfloat16 [2048, 128], replicated
The draws below stay inside these ranges and needn't reach their ends.
All inputs are finite; a program needn't handle non-finite values.
Results may differ from the reference program's by a relative error of at most 0.0075.
Values may be sent and summed in bfloat16 or wider, within the bound.
No kernel may reach another device: no remote copies, remote signals or barrier semaphores. Data moves between devices by JAX's collectives and lax.ppermute only.
A program may use at most 128 MiB of HBM per device.

```python
import jax
import jax.numpy as jnp
from jax import lax

EXPERTS = 128
D_MODEL = 2048
D_EXPERT = 768


def raised(result, rng, source, target, blocks, factor):
    def block_of(position):
        return (jnp.arange(result.shape[position]) // (result.shape[position] // blocks)).reshape((-1,) + (1,) * (result.ndim - 1 - position))

    near = jax.random.permutation(rng, blocks)[block_of(target)]
    other_side = (block_of(target) + blocks // 2) % blocks
    return jnp.where((block_of(source) == near) | (block_of(source) == other_side), factor * result, result)


def levels(rng, shape, split, smallest, largest):
    gain = 1.0
    for axis_at, blocks in split:
        draws = jax.random.uniform(jax.random.fold_in(jax.random.fold_in(rng, 6), axis_at), (blocks,), jnp.float32, smallest / len(split), largest / len(split))
        gain = gain * jnp.repeat(jnp.exp(draws), shape[axis_at] // blocks).reshape((-1,) + (1,) * (len(shape) - 1 - axis_at))
    return gain


def scatter_about(rng, shape, deviation, most, split=(), kind=jnp.bfloat16):
    entries = jax.random.normal(rng, shape, jnp.float32) * deviation
    if len(split) > 0:
        entries = levels(rng, shape, split, -0.22, 0.18) * entries
    return jnp.clip(entries, min=-most, max=most).astype(kind)


def heavy_noise(key, shape, scale, most, shards, heavy, kind=jnp.bfloat16):
    values = scale * jax.random.normal(key, shape, jnp.float32)
    if shards:
        values = values * levels(key, shape, shards, -0.22, 0.18)
    return jnp.clip(raised(values, jax.random.fold_in(key, 3), *heavy), -most, most).astype(kind)


def setup_inputs(seed: int = 0) -> dict:
    splits = jax.random.split(jax.random.key(seed), 7)
    train_gate = heavy_noise(splits[0], (EXPERTS, D_MODEL, D_EXPERT), D_MODEL ** -0.5, 0.25, ((0, 4), (1, 32)), (1, 2, 32, 2.75), jnp.float32)
    other_gate = scatter_about(splits[1], (EXPERTS, D_MODEL, D_EXPERT), (D_MODEL * 4) ** -0.5, 0.0625, ((0, 4), (1, 32)))
    train_up = heavy_noise(splits[2], (EXPERTS, D_MODEL, D_EXPERT), D_MODEL ** -0.5, 0.25, ((0, 4), (1, 32)), (1, 2, 32, 2.75), jnp.float32)
    other_up = scatter_about(splits[3], (EXPERTS, D_MODEL, D_EXPERT), (D_MODEL * 4) ** -0.5, 0.0625, ((0, 4), (1, 32)))
    router_weight = scatter_about(splits[4], (D_MODEL, EXPERTS), D_MODEL ** -0.5, 0.125, ((0, 32), (1, 4)), jnp.float32)
    router_gain = jnp.clip(1.0 + 0.15 * jax.random.normal(splits[5], (D_MODEL,), jnp.float32), 0.25, 1.75)
    return {"train_gate": train_gate, "other_gate": other_gate, "train_up": train_up, "other_up": other_up, "router_weight": router_weight, "router_gain": router_gain}


def reference(train_gate, other_gate, train_up, other_up, router_weight, router_gain):
    latest_gate = train_gate + other_gate.astype(jnp.float32)
    latest_up = train_up + other_up.astype(jnp.float32)
    scale_gate = jnp.sqrt(lax.optimization_barrier(jnp.sum(latest_gate * latest_gate, axis=1)))
    ready_gate = (latest_gate / jnp.expand_dims(scale_gate, 1)).astype(jnp.bfloat16)
    scale_up = jnp.sqrt(lax.optimization_barrier(jnp.sum(latest_up * latest_up, axis=1)))
    ready_up = (latest_up / jnp.expand_dims(scale_up, 1)).astype(jnp.bfloat16)
    serve_router = (router_weight * router_gain[:, None]).astype(jnp.bfloat16)
    return (ready_gate, ready_up, scale_gate, scale_up, serve_router)
```

```python
import jax
import jax.numpy as jnp
from jax import lax
from jax.sharding import PartitionSpec as P


def regrouped(train, other):
    latest = (train + other.astype(jnp.float32)).astype(jnp.bfloat16)
    return lax.all_to_all(latest, "zero", split_axis=0, concat_axis=1, tiled=True)


def normalised(pieces):
    wide = pieces.astype(jnp.float32)
    scale = jnp.sqrt(jnp.sum(wide * wide, axis=1))
    return (wide / scale[:, None, :]).astype(jnp.bfloat16), scale


def body(train_gate, other_gate, train_up, other_up, router_weight, router_gain):
    gate = regrouped(train_gate, other_gate)
    up = regrouped(train_up, other_up)
    part_router = (router_weight * router_gain[:, None]).astype(jnp.bfloat16)
    serve_router = lax.all_gather(part_router, "zero", axis=0, tiled=True)
    serve_router = lax.all_gather(serve_router, "bank", axis=1, tiled=True)
    ready_gate, scale_gate = normalised(gate)
    ready_up, scale_up = normalised(up)
    return (ready_gate, ready_up, scale_gate, scale_up, serve_router)


def solution(mesh):
    placed = (
        P("bank", "zero", None),
        P("bank", "zero", None),
        P("bank", "zero", None),
        P("bank", "zero", None),
        P("zero", "bank"),
        P("zero"),
    )
    return jax.shard_map(
        body,
        mesh=mesh,
        in_specs=placed,
        out_specs=(
            P(("bank", "zero"), None, None),
            P(("bank", "zero"), None, None),
            P(("bank", "zero"), None),
            P(("bank", "zero"), None),
            P(),
        ),
        check_vma=False,
    )
```

```python
import jax
import jax.numpy as jnp
from jax import lax
from jax.experimental import pallas as pl
from jax.experimental.pallas import tpu as pltpu
from jax.sharding import PartitionSpec as P

DESTS = 4


def latest_kernel(train_gate, other_gate, train_up, other_up, out):
    width = train_gate.shape[-1]
    out[:, :, :width] = (train_gate[...] + other_gate[...].astype(jnp.float32)).astype(jnp.bfloat16)
    out[:, :, width:] = (train_up[...] + other_up[...].astype(jnp.float32)).astype(jnp.bfloat16)


def latest_pieces(train_gate, other_gate, train_up, other_up):
    experts, rows, width = train_gate.shape
    block = pl.BlockSpec((DESTS, rows, width), lambda i: (i, 0, 0))
    return pl.pallas_call(
        latest_kernel,
        grid=(experts // DESTS,),
        in_specs=[block] * 4,
        out_specs=pl.BlockSpec((DESTS, rows, 2 * width), lambda i: (i, 0, 0)),
        out_shape=jax.ShapeDtypeStruct((experts, rows, 2 * width), jnp.bfloat16),
        name="latest_pieces",
    )(train_gate, other_gate, train_up, other_up)


LANES = 128
STEP = 256


def ready_kernel(pieces, ready, scale):
    rows = pieces.shape[0]
    for lane in range(0, pieces.shape[1], LANES):
        cols = pl.ds(lane, LANES)

        def squares(i, total):
            wide = pieces[pl.ds(i * STEP, STEP), cols].astype(jnp.float32)
            return total + jnp.sum((wide * wide).reshape(STEP // 8, 8, LANES), axis=0)

        total = lax.fori_loop(0, rows // STEP, squares, jnp.zeros((8, LANES), jnp.float32), unroll=True)
        root = jnp.sqrt(jnp.sum(total, axis=0, keepdims=True))
        scale[:, cols] = root
        inverse = 1.0 / root

        def scaled(i, carry):
            wide = pieces[pl.ds(i * STEP, STEP), cols].astype(jnp.float32)
            ready[0, pl.ds(i * STEP, STEP), cols] = (wide * inverse).astype(jnp.bfloat16)
            return carry

        lax.fori_loop(0, rows // STEP, scaled, 0, unroll=True)


BLOCK = 256


def ready_part(pieces, part):
    rows, width = pieces.shape[0], pieces.shape[1] // 2
    first = part * (width // BLOCK)
    return pl.pallas_call(
        ready_kernel,
        grid=(width // BLOCK,),
        in_specs=[pl.BlockSpec((rows, BLOCK), lambda j: (0, first + j))],
        out_specs=[
            pl.BlockSpec((1, rows, BLOCK), lambda j: (0, 0, j)),
            pl.BlockSpec((1, BLOCK), lambda j: (0, j)),
        ],
        out_shape=[
            jax.ShapeDtypeStruct((1, rows, width), jnp.bfloat16),
            jax.ShapeDtypeStruct((1, width), jnp.float32),
        ],
        name="ready_part",
    )(pieces)


def paired(array, axis, bit):
    size = lax.axis_size(axis)
    other = lax.ppermute(array, axis, [(i, i ^ bit) for i in range(size)])
    high = (lax.axis_index(axis) & bit) != 0
    return jnp.where(high, other, array), jnp.where(high, array, other)


def gathered_router(router):
    for bit in (1, 2, 4, 8, 16):
        router = jnp.concatenate(paired(router, "zero", bit), axis=1)
    router = jnp.stack(paired(router, "bank", 2))
    router = jnp.concatenate(paired(router, "bank", 1), axis=1)
    return router.reshape(-1, router.shape[-1]).T


def body(train_gate, other_gate, train_up, other_up, router_weight, router_gain):
    pieces = latest_pieces(train_gate, other_gate, train_up, other_up)
    served = lax.all_to_all(pieces, "zero", split_axis=0, concat_axis=1, tiled=True)
    served = served.reshape(served.shape[1], served.shape[2])
    router = (router_weight.T * router_gain[None, :]).astype(jnp.bfloat16)
    serve_router = gathered_router(router)
    ready_gate, scale_gate = ready_part(served, 0)
    ready_up, scale_up = ready_part(served, 1)
    return (ready_gate, ready_up, scale_gate, scale_up, serve_router)


def solution(mesh):
    placed = (
        P("bank", "zero", None),
        P("bank", "zero", None),
        P("bank", "zero", None),
        P("bank", "zero", None),
        P("zero", "bank"),
        P("zero"),
    )
    return jax.shard_map(
        body,
        mesh=mesh,
        in_specs=placed,
        out_specs=(
            P(("bank", "zero"), None, None),
            P(("bank", "zero"), None, None),
            P(("bank", "zero"), None),
            P(("bank", "zero"), None),
            P(),
        ),
        check_vma=False,
    )
```

```python
import jax
import jax.numpy as jnp
from jax import lax
from jax.experimental import pallas as pl
from jax.experimental.pallas import tpu as pltpu
from jax.sharding import PartitionSpec as P

LANES = 128
DESTS = 2
BUFFERS = 3
MIB = 1 << 20


def latest_kernel(train_gate, other_gate, train_up, other_up, out):
    experts, rows, width = train_gate.shape
    half = rows * width // LANES
    block = pl.BlockSpec((DESTS, rows, width), lambda i: (i, 0, 0), pipeline_mode=pl.Buffered(BUFFERS))

    def step(train_gate, other_gate, train_up, other_up):
        i = pl.program_id(0)
        for start, train, other in ((0, train_gate, other_gate), (half, train_up, other_up)):
            for d in range(DESTS):
                for at in range(width // LANES):
                    cols = pl.ds(at * LANES, LANES)
                    latest = train[d, :, cols] + other[d, :, cols].astype(jnp.float32)
                    out[i * DESTS + d, start + at * rows : start + (at + 1) * rows, :] = latest.astype(jnp.bfloat16)

    pltpu.emit_pipeline(step, grid=(experts // DESTS,), in_specs=[block] * 4)(
        train_gate, other_gate, train_up, other_up
    )


def latest_pieces(arrays, total):
    experts = arrays[0].shape[0]
    return pl.pallas_call(
        latest_kernel,
        in_specs=[pl.BlockSpec(memory_space=pltpu.HBM)] * 4,
        out_specs=pl.BlockSpec(memory_space=pltpu.VMEM),
        out_shape=pltpu.VMEM((experts, total, LANES), jnp.bfloat16),
        compiler_params=pltpu.CompilerParams(vmem_limit_bytes=24 * MIB),
        name="latest_pieces",
    )(*(pltpu.with_memory_space_constraint(array, pltpu.HBM) for array in arrays))


def routed_kernel(router, pieces, out):
    out[:, out.shape[1] - router.shape[0] :, :] = jnp.broadcast_to(router[...][None], (out.shape[0], *router.shape))


def routed_pieces(router, pieces):
    return pl.pallas_call(
        routed_kernel,
        in_specs=[pl.BlockSpec(memory_space=pltpu.VMEM)] * 2,
        out_specs=pl.BlockSpec(memory_space=pltpu.VMEM),
        out_shape=pltpu.VMEM(pieces.shape, pieces.dtype),
        input_output_aliases={1: 0},
        compiler_params=pltpu.CompilerParams(vmem_limit_bytes=24 * MIB),
        name="routed_pieces",
    )(router, pieces)


def ready_block(pieces, ready, scale):
    sources, rows, _ = pieces.shape
    total = jnp.zeros((rows, LANES), jnp.float32)
    for s in range(sources):
        wide = pieces[s].astype(jnp.float32)
        total = total + wide * wide
    root = jnp.sqrt(jnp.sum(total, axis=0, keepdims=True))
    scale[...] = root
    inverse = jnp.broadcast_to(1.0 / root, (rows, LANES))
    for s in range(sources):
        wide = pieces[s].astype(jnp.float32)
        ready[0, s * rows : (s + 1) * rows, :] = (wide * inverse).astype(jnp.bfloat16)


def ready_kernel(pieces, ready_gate, ready_up, scale_gate, scale_up):
    sources = pieces.shape[0]
    rows, width = ready_gate.shape[1] // sources, ready_gate.shape[2]
    blocks = width // LANES

    def step(block, gate, up, root_gate, root_up):
        j = pl.program_id(0)

        @pl.when(j < blocks)
        def _():
            ready_block(block, gate, root_gate)

        @pl.when(j >= blocks)
        def _():
            ready_block(block, up, root_up)

    gate = lambda j: jnp.minimum(j, blocks - 1)
    up = lambda j: jnp.maximum(j - blocks, 0)
    pltpu.emit_pipeline(
        step,
        grid=(2 * blocks,),
        in_specs=[
            pl.BlockSpec((sources, rows, LANES), lambda j: (0, j, 0), pipeline_mode=pl.Buffered(BUFFERS))
        ],
        out_specs=[
            pl.BlockSpec((1, sources * rows, LANES), lambda j: (0, 0, gate(j))),
            pl.BlockSpec((1, sources * rows, LANES), lambda j: (0, 0, up(j))),
            pl.BlockSpec((1, LANES), lambda j: (0, gate(j))),
            pl.BlockSpec((1, LANES), lambda j: (0, up(j))),
        ],
    )(pieces, ready_gate, ready_up, scale_gate, scale_up)


def ready_parts(pieces, rows, width):
    ready = jax.ShapeDtypeStruct((1, pieces.shape[0] * rows, width), jnp.bfloat16)
    scale = jax.ShapeDtypeStruct((1, width), jnp.float32)
    return pl.pallas_call(
        ready_kernel,
        in_specs=[pl.BlockSpec(memory_space=pltpu.HBM)],
        out_specs=[pl.BlockSpec(memory_space=pltpu.HBM)] * 4,
        out_shape=[ready, ready, scale, scale],
        compiler_params=pltpu.CompilerParams(vmem_limit_bytes=24 * MIB),
        name="ready_parts",
    )(pieces)


def own_router_kernel(pieces, own, sem):
    cols = own.shape[1]
    copy = pltpu.make_async_copy(pieces.at[:, pl.ds(pieces.shape[1] - cols, cols)], own, sem)
    copy.start()
    copy.wait()


def own_router(pieces, cols):
    return pl.pallas_call(
        own_router_kernel,
        in_specs=[pl.BlockSpec(memory_space=pltpu.HBM)],
        out_specs=pl.BlockSpec(memory_space=pltpu.VMEM),
        out_shape=pltpu.VMEM((pieces.shape[0], cols, LANES), pieces.dtype),
        scratch_shapes=[pltpu.SemaphoreType.DMA],
        compiler_params=pltpu.CompilerParams(vmem_limit_bytes=4 * MIB),
        name="own_router",
    )(pieces)


def swapped(array, axis, bit):
    size = lax.axis_size(axis)
    return lax.ppermute(array, axis, [(i, i ^ bit) for i in range(size)])


def router_kernel(core, own, other, out):
    sources, cols, _ = own.shape
    rows = LANES // 2
    first = core[0] == 0
    for s in range(sources):
        mine, theirs = own[s].astype(jnp.float32), other[s].astype(jnp.float32)
        even, odd = jnp.where(first, mine, theirs), jnp.where(first, theirs, mine)
        tall = jnp.concatenate([even[:, :rows], odd[:, :rows], even[:, rows:], odd[:, rows:]], axis=0)
        out[s * rows : (s + 1) * rows, :] = tall.T.astype(jnp.bfloat16)


def served_router(own, other):
    sources, cols, _ = own.shape
    core = (lax.axis_index("bank") & 1).astype(jnp.int32).reshape(1)
    return pl.pallas_call(
        router_kernel,
        in_specs=[
            pl.BlockSpec(memory_space=pltpu.SMEM),
            pl.BlockSpec(memory_space=pltpu.VMEM),
            pl.BlockSpec(memory_space=pltpu.VMEM),
        ],
        out_specs=pl.BlockSpec(memory_space=pltpu.VMEM),
        out_shape=jax.ShapeDtypeStruct((sources * LANES // 2, 4 * cols), jnp.bfloat16),
        compiler_params=pltpu.CompilerParams(vmem_limit_bytes=8 * MIB),
        name="served_router",
    )(core, own, other)


def body(train_gate, other_gate, train_up, other_up, router_weight, router_gain):
    experts, rows, width = train_gate.shape
    router = (router_weight.T * router_gain[None, :]).astype(jnp.bfloat16)
    cols = router.shape[0]
    across = swapped(router, "bank", 2)
    total = 2 * rows * width // LANES + cols
    pieces = latest_pieces((train_gate, other_gate, train_up, other_up), total)
    low = (lax.axis_index("bank") & 2) == 0
    router = jnp.concatenate([jnp.where(low, router, across), jnp.where(low, across, router)], axis=1)
    pieces = routed_pieces(router, pieces)
    served = lax.all_to_all(pieces, "zero", split_axis=0, concat_axis=0, tiled=True)
    served = pltpu.with_memory_space_constraint(served, pltpu.HBM)
    own = own_router(served, cols)
    other = swapped(own, "bank", 1)
    ready_gate, ready_up, scale_gate, scale_up = ready_parts(served, rows, width)
    serve_router = served_router(own, other)
    return (ready_gate, ready_up, scale_gate, scale_up, serve_router)


def solution(mesh):
    placed = (
        P("bank", "zero", None),
        P("bank", "zero", None),
        P("bank", "zero", None),
        P("bank", "zero", None),
        P("zero", "bank"),
        P("zero"),
    )
    return jax.shard_map(
        body,
        mesh=mesh,
        in_specs=placed,
        out_specs=(
            P(("bank", "zero"), None, None),
            P(("bank", "zero"), None, None),
            P(("bank", "zero"), None),
            P(("bank", "zero"), None),
            P(),
        ),
        check_vma=False,
    )
```

```python
import jax
import jax.numpy as jnp
from jax import lax
from jax.experimental import pallas as pl
from jax.experimental.pallas import tpu as pltpu
from jax.sharding import PartitionSpec as P

LANES = 128
DESTS = 4
SOURCES = 2
MIB = 1 << 20


def in_hbm(array):
    return pltpu.with_memory_space_constraint(array, pltpu.HBM)


def in_vmem(array):
    return pltpu.with_memory_space_constraint(array, pltpu.VMEM)


def latest_kernel(train_gate, other_gate, train_up, other_up, out, trains, others, sems):
    experts, rows, width = train_gate.shape
    blocks = width // LANES
    pairs = ((train_gate, trains.at[0]), (other_gate, others.at[0]), (train_up, trains.at[1]), (other_up, others.at[1]))

    def copies(i):
        at = pl.ds(i * DESTS, DESTS)
        return [pltpu.make_async_copy(hbm.at[at], vmem.at[at], sems.at[i]) for hbm, vmem in pairs]

    for i in range(experts // DESTS):
        for copy in copies(i):
            copy.start()

    def step(i, carry):
        for copy in copies(i):
            copy.wait()
        for part in range(2):
            for d in range(DESTS):
                for at in range(blocks):
                    cols = pl.ds(at * LANES, LANES)
                    e = i * DESTS + d
                    latest = trains[part, e, :, cols] + others[part, e, :, cols].astype(jnp.float32)
                    start = (part * blocks + at) * rows
                    out[e, start : start + rows, :] = latest.astype(jnp.bfloat16)
        return carry

    lax.fori_loop(0, experts // DESTS, step, 0)


def latest_pieces(arrays, total):
    experts, rows, width = arrays[0].shape
    return pl.pallas_call(
        latest_kernel,
        in_specs=[pl.BlockSpec(memory_space=pltpu.HBM)] * 4,
        out_specs=pl.BlockSpec(memory_space=pltpu.VMEM),
        out_shape=pltpu.VMEM((experts, total, LANES), jnp.bfloat16),
        scratch_shapes=[
            pltpu.VMEM((2, experts, rows, width), jnp.float32),
            pltpu.VMEM((2, experts, rows, width), jnp.bfloat16),
            pltpu.SemaphoreType.DMA((experts // DESTS,)),
        ],
        compiler_params=pltpu.CompilerParams(vmem_limit_bytes=40 * MIB),
        name="latest_pieces",
    )(*(in_hbm(array) for array in arrays))


def routed_kernel(router, pieces, out):
    out[:, out.shape[1] - router.shape[0] :, :] = jnp.broadcast_to(router[...][None], (out.shape[0], *router.shape))


def routed_pieces(router, pieces):
    return pl.pallas_call(
        routed_kernel,
        in_specs=[pl.BlockSpec(memory_space=pltpu.VMEM)] * 2,
        out_specs=pl.BlockSpec(memory_space=pltpu.VMEM),
        out_shape=pltpu.VMEM(pieces.shape, pieces.dtype),
        input_output_aliases={1: 0},
        compiler_params=pltpu.CompilerParams(vmem_limit_bytes=24 * MIB),
        name="routed_pieces",
    )(router, pieces)


def ready_kernel(pieces, ready_gate, ready_up, scale_gate, scale_up, own, buffer, sems):
    sources = pieces.shape[0]
    rows, width = ready_gate.shape[1] // sources, ready_gate.shape[2]
    blocks = width // LANES
    for part, (ready, scale) in enumerate(((ready_gate, scale_gate), (ready_up, scale_up))):
        starts = [(part * blocks + at) * rows for at in range(blocks)]
        inverses = []
        for at, start in enumerate(starts):
            total = jnp.zeros((rows, LANES), jnp.float32)
            for s in range(sources):
                wide = pieces[s, start : start + rows, :].astype(jnp.float32)
                total = total + wide * wide
            root = jnp.sqrt(jnp.sum(total, axis=0, keepdims=True))
            scale[:, at * LANES : (at + 1) * LANES] = root
            inverses.append(1.0 / root)

        def step(g, carry):
            for s in range(SOURCES):
                lines = pl.ds(pl.multiple_of((g * SOURCES + s) * rows, rows), rows)
                for at, start in enumerate(starts):
                    wide = pieces[g * SOURCES + s, start : start + rows, :].astype(jnp.float32)
                    buffer[part, lines, at * LANES : (at + 1) * LANES] = (wide * inverses[at]).astype(jnp.bfloat16)
            lines = pl.ds(pl.multiple_of(g * SOURCES * rows, SOURCES * rows), SOURCES * rows)
            pltpu.make_async_copy(buffer.at[part, lines], ready.at[0, lines], sems.at[part]).start()
            return carry

        lax.fori_loop(0, sources // SOURCES, step, 0)
    own[...] = pieces[:, 2 * blocks * rows :, :]
    for part, ready in enumerate((ready_gate, ready_up)):
        pltpu.make_async_copy(buffer.at[part], ready.at[0], sems.at[part]).wait()


def ready_parts(pieces, rows, width):
    sources, total, _ = pieces.shape
    ready = jax.ShapeDtypeStruct((1, sources * rows, width), jnp.bfloat16)
    scale = jax.ShapeDtypeStruct((1, width), jnp.float32)
    own = pltpu.VMEM((sources, total - 2 * rows * width // LANES, LANES), pieces.dtype)
    return pl.pallas_call(
        ready_kernel,
        in_specs=[pl.BlockSpec(memory_space=pltpu.VMEM)],
        out_specs=[pl.BlockSpec(memory_space=pltpu.HBM)] * 2 + [pl.BlockSpec(memory_space=pltpu.VMEM)] * 3,
        out_shape=[ready, ready, scale, scale, own],
        scratch_shapes=[
            pltpu.VMEM((2, sources * rows, width), jnp.bfloat16),
            pltpu.SemaphoreType.DMA((2,)),
        ],
        compiler_params=pltpu.CompilerParams(vmem_limit_bytes=24 * MIB),
        name="ready_parts",
    )(in_vmem(pieces))


def swapped(array, axis, bit):
    size = lax.axis_size(axis)
    return lax.ppermute(array, axis, [(i, i ^ bit) for i in range(size)])


def packed_router(weight, across, gain):
    bank = lax.axis_index("bank")
    parts = [(w * gain[:, None]).astype(jnp.bfloat16) for w in (weight, across)]
    low, even = (bank & 2) == 0, (bank & 1) == 0
    parts = [jnp.where(low, parts[0], parts[1]), jnp.where(low, parts[1], parts[0])]
    half = weight.shape[0] // 2
    groups = []
    for part in parts:
        groups += [jnp.where(even, part[:half], part[half:]), jnp.where(even, part[half:], part[:half])]
    return jnp.concatenate(groups, axis=1)


def router_kernel(odd, own, other, out):
    sources, half, _ = own.shape
    lane = lax.broadcasted_iota(jnp.int32, (half, LANES), 1)
    even_lanes = (lane // (LANES // 4)) % 2 == 0
    mine = even_lanes == (odd[0] == 0)
    for s in range(sources):
        a, b = own[s].astype(jnp.float32), other[s].astype(jnp.float32)
        first, second = jnp.where(mine, a, b), jnp.where(mine, b, a)
        left = pltpu.roll(second, LANES - LANES // 4, 1)
        right = pltpu.roll(second, LANES // 4, 1)
        out[2 * s * half : (2 * s + 1) * half, :] = first.astype(jnp.bfloat16)
        out[(2 * s + 1) * half : 2 * (s + 1) * half, :] = jnp.where(even_lanes, left, right).astype(jnp.bfloat16)


def served_router(own, other):
    sources, half, _ = own.shape
    odd = (lax.axis_index("bank") & 1).astype(jnp.int32).reshape(1)
    return pl.pallas_call(
        router_kernel,
        in_specs=[
            pl.BlockSpec(memory_space=pltpu.SMEM),
            pl.BlockSpec(memory_space=pltpu.VMEM),
            pl.BlockSpec(memory_space=pltpu.VMEM),
        ],
        out_specs=pl.BlockSpec(memory_space=pltpu.VMEM),
        out_shape=jax.ShapeDtypeStruct((2 * sources * half, LANES), jnp.bfloat16),
        compiler_params=pltpu.CompilerParams(vmem_limit_bytes=8 * MIB),
        name="served_router",
    )(odd, own, other)


def body(train_gate, other_gate, train_up, other_up, router_weight, router_gain):
    experts, rows, width = train_gate.shape
    across = swapped(router_weight.T, "bank", 2).T
    total = 2 * rows * width // LANES + rows // 2
    pieces = latest_pieces((train_gate, other_gate, train_up, other_up), total)
    pieces = routed_pieces(packed_router(router_weight, across, router_gain), pieces)
    served = lax.all_to_all(pieces, "zero", split_axis=0, concat_axis=0, tiled=True)
    ready_gate, ready_up, scale_gate, scale_up, own = ready_parts(served, rows, width)
    serve_router = served_router(own, swapped(own, "bank", 1))
    return (ready_gate, ready_up, scale_gate, scale_up, serve_router)


def solution(mesh):
    placed = (
        P("bank", "zero", None),
        P("bank", "zero", None),
        P("bank", "zero", None),
        P("bank", "zero", None),
        P("zero", "bank"),
        P("zero"),
    )
    return jax.shard_map(
        body,
        mesh=mesh,
        in_specs=placed,
        out_specs=(
            P(("bank", "zero"), None, None),
            P(("bank", "zero"), None, None),
            P(("bank", "zero"), None),
            P(("bank", "zero"), None),
            P(),
        ),
        check_vma=False,
    )
```
